16 devices in a mesh: data: 16 (over z, y, x, core).
Axes of the slice: x: 2, y: 2, z: 2, core: 2. Of those that a mesh axis runs over, the one named last changes fastest.
Arguments:
- tokens: bfloat16 [16384, 1280], P('data')
- targets: bfloat16 [16384, 1280], P('data')
- w_in: bfloat16 [4, 1280, 5120], replicated
- w_out: bfloat16 [4, 5120, 1280], replicated
Outputs:
- output 1: float32 [4, 1280, 5120], P(None, 'data')
- output 2: float32 [4, 5120, 1280], P(None, 'data')
All inputs are finite; a program needn't handle non-finite values.
Results may differ from the reference program's by a relative error of at most 0.00447066.
Values are sent between devices in bfloat16 or wider.
A program may use at most 1 GiB of HBM per device.

```python
import jax
import jax.numpy as jnp
from jax import lax

D = 1280
FF = 5120
LAYERS = 4
TOKENS_DEV = 1024
DATA = 16
TOKENS = TOKENS_DEV * DATA


def setup_inputs(seed: int = 0) -> dict:
    key_root = jax.random.key(seed)
    key_tok, key_tgt, key_in, key_out = jax.random.split(key_root, 4)
    tokens = jax.random.normal(key_tok, (TOKENS, D), jnp.float32).astype(jnp.bfloat16)
    targets = (2.0 * jax.random.normal(key_tgt, (TOKENS, D), jnp.float32)).astype(jnp.bfloat16)
    w_in = (jax.random.normal(key_in, (LAYERS, D, FF), jnp.float32) * (D ** -0.5)).astype(jnp.bfloat16)
    w_out = (jax.random.normal(key_out, (LAYERS, FF, D), jnp.float32) * (0.5 * FF ** -0.5)).astype(jnp.bfloat16)
    return {"tokens": tokens, "targets": targets, "w_in": w_in, "w_out": w_out}


def gelu_act(pre_f32):
    return jax.nn.gelu(pre_f32, approximate=True)


def layer_forward(hidden, weights):
    w_first, w_second = weights
    pre_act = jnp.dot(hidden, w_first, preferred_element_type=jnp.float32).astype(jnp.bfloat16)
    act_out = gelu_act(pre_act.astype(jnp.float32)).astype(jnp.bfloat16)
    branch = jnp.dot(act_out, w_second, preferred_element_type=jnp.float32)
    new_hidden = (hidden.astype(jnp.float32) + branch).astype(jnp.bfloat16)
    return new_hidden, (hidden, pre_act, act_out)


def layer_backward(grad_h, saved_items):
    hidden, pre_act, act_out, w_first, w_second = saved_items
    grad_second = jnp.dot(act_out.T, grad_h, preferred_element_type=jnp.float32)
    grad_act = jnp.dot(grad_h, w_second.T, preferred_element_type=jnp.float32).astype(jnp.bfloat16)
    _, pullback = jax.vjp(gelu_act, pre_act.astype(jnp.float32))
    grad_pre = pullback(grad_act.astype(jnp.float32))[0].astype(jnp.bfloat16)
    grad_first = jnp.dot(hidden.T, grad_pre, preferred_element_type=jnp.float32)
    grad_below = jnp.dot(grad_pre, w_first.T, preferred_element_type=jnp.float32)
    new_grad = (grad_h.astype(jnp.float32) + grad_below).astype(jnp.bfloat16)
    return new_grad, (grad_first, grad_second)


def block_grads(tok_rows, tgt_rows, w_in, w_out):
    top_hidden, saved_fwd = lax.scan(layer_forward, tok_rows, (w_in, w_out))
    grad_top = ((top_hidden.astype(jnp.float32) - tgt_rows.astype(jnp.float32)) * (TOKENS ** -0.5)).astype(jnp.bfloat16)
    _, layer_grads = lax.scan(layer_backward, grad_top, (saved_fwd[0], saved_fwd[1], saved_fwd[2], w_in, w_out), reverse=True)
    return layer_grads


def reference(tokens, targets, w_in, w_out):
    tok_blocks = tokens.reshape(DATA, TOKENS_DEV, D)
    tgt_blocks = targets.reshape(DATA, TOKENS_DEV, D)

    def accumulate(carry, row_pair):
        grad_first, grad_second = block_grads(row_pair[0], row_pair[1], w_in, w_out)
        return (carry[0] + grad_first, carry[1] + grad_second), None

    zero_sums = (jnp.zeros((LAYERS, D, FF), jnp.float32), jnp.zeros((LAYERS, FF, D), jnp.float32))
    (sum_first, sum_second), _ = lax.scan(accumulate, zero_sums, (tok_blocks, tgt_blocks))
    return sum_first, sum_second
```

```python
import jax
import jax.numpy as jnp
from jax import lax
from jax.sharding import PartitionSpec as P


CORE, X, Y, Z = 0, 1, 2, 3


def gelu_act(pre_f32):
    return jax.nn.gelu(pre_f32, approximate=True)


def swap(v, bit, n=16):
    return lax.ppermute(v, "data", [(d, d ^ (1 << bit)) for d in range(n)])


def pick(v, pos, idx):
    return lax.dynamic_index_in_dim(v, idx, pos, keepdims=True)


def exchange_sum(keep_terms, send_terms, order, bits):
    terms = keep_terms
    for bit in order:
        pos = 3 - bit
        send = sum(pick(t, pos, 1 - bits[bit]) for t in terms)
        recv = swap(send, bit)
        terms = [pick(t, pos, bits[bit]) for t in terms] + [recv]
    return sum(terms)


def solution(mesh):
    data_size = mesh.shape["data"]

    def reduce_matrix(lhs, rhs, sub, bits, cuts):
        t = lhs.shape[0]
        lhs6 = lhs.reshape(t, 2, 2, 2, 2, sub)
        halves = []
        for which in (1 - bits[CORE], bits[CORE]):
            part = lax.dynamic_index_in_dim(lhs6, which, 4, keepdims=True)
            part = part.reshape(t, 8 * sub)
            halves.append(jnp.einsum("tf,td->fd", part, rhs, preferred_element_type=jnp.float32))
        recv = swap(halves[0], CORE)
        mine = halves[1] + recv
        mine = mine.reshape(2, 2, 2, 1, sub, rhs.shape[1])
        outs = []
        for i, (lo, hi) in enumerate(cuts):
            order = [(X, Y, Z), (Y, Z, X), (Z, X, Y)][i]
            outs.append(exchange_sum([mine[..., lo:hi]], None, order, bits).reshape(sub, hi - lo))
        return jnp.concatenate(outs, axis=1)

    def local_grads(tokens, targets, w_in, w_out):
        layers = w_in.shape[0]
        scale = (tokens.shape[0] * data_size) ** -0.5
        me = lax.axis_index("data")
        bits = [(me >> b) & 1 for b in range(4)]
        hidden = tokens
        saved_fwd = []
        for layer in range(layers):
            pre_act = jnp.dot(hidden, w_in[layer], preferred_element_type=jnp.float32).astype(jnp.bfloat16)
            act_out = gelu_act(pre_act.astype(jnp.float32)).astype(jnp.bfloat16)
            branch = jnp.dot(act_out, w_out[layer], preferred_element_type=jnp.float32)
            saved_fwd.append((hidden, pre_act, act_out))
            hidden = (hidden.astype(jnp.float32) + branch).astype(jnp.bfloat16)
        grad_h = ((hidden.astype(jnp.float32) - targets.astype(jnp.float32)) * scale).astype(jnp.bfloat16)
        shares_first = [None] * layers
        shares_second = [None] * layers
        for layer in reversed(range(layers)):
            hidden_in, pre_act, act_out = saved_fwd[layer]
            shares_second[layer] = reduce_matrix(act_out, grad_h, 320, bits, [(0, 512), (512, 896), (896, 1280)])
            grad_act = jnp.einsum("td,fd->tf", grad_h, w_out[layer], preferred_element_type=jnp.float32).astype(jnp.bfloat16)
            _, pullback = jax.vjp(gelu_act, pre_act.astype(jnp.float32))
            grad_pre = pullback(grad_act.astype(jnp.float32))[0].astype(jnp.bfloat16)
            shares_first[layer] = reduce_matrix(hidden_in, grad_pre, 80, bits, [(0, 1792), (1792, 3456), (3456, 5120)])
            if layer > 0:
                grad_below = jnp.einsum("tf,df->td", grad_pre, w_in[layer], preferred_element_type=jnp.float32)
                grad_h = (grad_h.astype(jnp.float32) + grad_below).astype(jnp.bfloat16)
        return jnp.stack(shares_first), jnp.stack(shares_second)

    tok_spec = P("data", None)
    grad_spec = P(None, "data", None)
    return jax.shard_map(local_grads, mesh=mesh, in_specs=(tok_spec, tok_spec, P(), P()), out_specs=(grad_spec, grad_spec), check_vma=False)
```

```python
import functools

import jax
import jax.numpy as jnp
from jax import lax
from jax.experimental import pallas as pl
from jax.experimental.pallas import tpu as pltpu
from jax.sharding import PartitionSpec as P

BF = jnp.bfloat16
F32 = jnp.float32
MESH = pl.DeviceIdType.MESH
VMEM_LIMIT = 67043328

SQRT_2_OVER_PI = 0.7978845608028654
C1 = SQRT_2_OVER_PI * 0.044715


def gelu_parts(x):
    x2 = x * x
    p = C1 * x2 + SQRT_2_OVER_PI
    t = jnp.tanh(x * p)
    s = 0.5 * t + 0.5
    return x2, t, s


def gelu(x):
    _, _, s = gelu_parts(x)
    return x * s


def gelu_grad(x):
    x2, t, s = gelu_parts(x)
    q = (3.0 * C1) * x2 + SQRT_2_OVER_PI
    return s + (0.5 * x) * (1.0 - t * t) * q


def fwd_kernel(scale, chunk, x_ref, t_ref, win_ref, wout_ref, u_ref, at_ref, ht_ref, g_ref, h, acc):
    layer, j = pl.program_id(0), pl.program_id(1)
    last = pl.num_programs(1) - 1
    tokens = h.shape[0]
    sub = ht_ref.shape[1]

    @pl.when((layer == 0) & (j == 0))
    def _():
        h[...] = x_ref[...]

    @pl.when(j == 0)
    def _():
        acc[...] = h[...].astype(F32)

    ht_ref[0] = h[:, pl.ds(pl.multiple_of(j * sub, sub), sub)].T
    for c in range(tokens // chunk):
        rows = slice(c * chunk, (c + 1) * chunk)
        u = jnp.dot(h[rows], win_ref[0], preferred_element_type=F32).astype(BF)
        u_ref[0, rows] = u
        a = gelu(u.astype(F32)).astype(BF)
        at_ref[0, :, rows] = a.T
        acc[rows] += jnp.dot(a, wout_ref[0], preferred_element_type=F32)

    @pl.when(j == last)
    def _():
        h[...] = acc[...].astype(BF)

    @pl.when((j == last) & (layer == pl.num_programs(0) - 1))
    def _():
        g_ref[...] = ((h[...].astype(F32) - t_ref[...].astype(F32)) * scale).astype(BF)


def forward(tokens, targets, w_in, w_out, scale, ftile=512, chunk=512):
    t, d = tokens.shape
    layers, _, ff = w_in.shape
    nj = ff // ftile
    return pl.pallas_call(
        functools.partial(fwd_kernel, scale, chunk),
        grid=(layers, nj),
        in_specs=[
            pl.BlockSpec((t, d), lambda l, j: (0, 0)),
            pl.BlockSpec((t, d), lambda l, j: (0, 0)),
            pl.BlockSpec((1, d, ftile), lambda l, j: (l, 0, j)),
            pl.BlockSpec((1, ftile, d), lambda l, j: (l, j, 0)),
        ],
        out_specs=[
            pl.BlockSpec((1, t, ftile), lambda l, j: (l, 0, j)),
            pl.BlockSpec((1, ftile, t), lambda l, j: (l, j, 0)),
            pl.BlockSpec((1, d // nj, t), lambda l, j: (l, j, 0)),
            pl.BlockSpec((t, d), lambda l, j: (0, 0)),
        ],
        out_shape=[
            jax.ShapeDtypeStruct((layers, t, ff), BF),
            jax.ShapeDtypeStruct((layers, ff, t), BF),
            jax.ShapeDtypeStruct((layers, d, t), BF),
            jax.ShapeDtypeStruct((t, d), BF),
        ],
        scratch_shapes=[pltpu.VMEM((t, d), BF), pltpu.VMEM((t, d), F32)],
        compiler_params=pltpu.CompilerParams(
            dimension_semantics=("arbitrary", "arbitrary"), vmem_limit_bytes=VMEM_LIMIT
        ),
        name="forward",
    )(tokens, targets, w_in, w_out)


ORDERS = ((2, 1, 0), (1, 0, 2), (0, 2, 1))
NIT = 5


def block_index(fixed):
    return tuple(fixed.get(a, slice(None)) for a in range(3))


def bwd_kernel(
    layers, cuts2, cuts1,
    u_hbm, at_hbm, ht_hbm, g_hbm, win_hbm, wout_hbm,
    o1_hbm, o2_hbm,
    g, acc, ht, at, u, wi, wo, v,
    s2, s1, c2, c1, p2, p1, r2a, r2b, r2c, r1a, r1b, r1c,
    sem_g, sem_ht, sem_at, sem_e, sem_out,
    csend, crecv, ssend, srecv, credit,
):
    t, d = g.shape
    ff = u_hbm.shape[2]
    rows2, rows1 = p2.shape[4], p1.shape[4]
    own2 = ff // 16
    fw = ff // NIT
    sub = u.shape[2]
    nsub = fw // sub
    half = t // 2
    total = layers * NIT

    me = lax.axis_index("data")
    bc = lax.rem(me, 2)
    bx = lax.rem(lax.div(me, 2), 2)
    by = lax.rem(lax.div(me, 4), 2)
    bz = lax.div(me, 8)
    bits = (bz, by, bx)
    partner = tuple(me + (1 - 2 * b) * s for b, s in zip(bits, (8, 4, 2)))
    sibling = me + 1 - 2 * bc

    def flip(b, r):
        return 1 - b if r else b

    def owner(rz, ry, rx, rc):
        return 8 * flip(bz, rz) + 4 * flip(by, ry) + 2 * flip(bx, rx) + flip(bc, rc)

    def layer_of(it):
        return layers - 1 - lax.div(it, NIT)

    def at_copies(it):
        slot = lax.rem(it, 2)
        lyr, n = layer_of(it), lax.rem(it, NIT)
        out = []
        for rc in range(2):
            for b in range(8):
                o = owner(b >> 2, (b >> 1) & 1, b & 1, rc)
                row = pl.multiple_of(o * own2 + n * rows2, rows2)
                out.append(pltpu.make_async_copy(
                    at_hbm.at[lyr, pl.ds(row, rows2)], at.at[slot, rc, pl.ds(b * rows2, rows2)], sem_at.at[slot]))
        return out

    def at_wait(it):
        slot = lax.rem(it, 2)
        for rc in range(2):
            pltpu.make_async_copy(at_hbm.at[0, pl.ds(0, 8 * rows2)], at.at[slot, rc], sem_at.at[slot]).wait()

    def ht_copies(lyr, slot):
        out = []
        for rc in range(2):
            for b in range(8):
                o = owner(b >> 2, (b >> 1) & 1, b & 1, rc)
                row = pl.multiple_of(o * rows1, rows1)
                out.append(pltpu.make_async_copy(
                    ht_hbm.at[lyr, pl.ds(row, rows1)], ht.at[slot, rc, pl.ds(b * rows1, rows1)], sem_ht.at[slot]))
        return out

    def ht_wait(slot):
        for rc in range(2):
            pltpu.make_async_copy(ht_hbm.at[0, pl.ds(0, 8 * rows1)], ht.at[slot, rc], sem_ht.at[slot]).wait()

    def e_copies(m):
        slot = lax.rem(m, 2)
        lyr = layer_of(lax.div(m, nsub))
        col = pl.multiple_of(lax.rem(m, NIT * nsub) * sub, sub)
        return [
            pltpu.make_async_copy(u_hbm.at[lyr, :, pl.ds(col, sub)], u.at[slot], sem_e.at[0, slot]),
            pltpu.make_async_copy(wout_hbm.at[lyr, pl.ds(col, sub)], wo.at[slot], sem_e.at[1, slot]),
            pltpu.make_async_copy(win_hbm.at[lyr, :, pl.ds(col, sub)], wi.at[slot], sem_e.at[2, slot]),
        ]

    def start(copies):
        for c in copies:
            c.start()

    tiles = {
        2: dict(k=0, s=s2, c=c2, p=p2, r=(r2a, r2b, r2c), cuts=cuts2),
        1: dict(k=1, s=s1, c=c1, p=p1, r=(r1a, r1b, r1c), cuts=cuts1),
    }

    def core_copy(ti):
        k = ti["k"]
        return pltpu.make_async_remote_copy(
            src_ref=ti["s"], dst_ref=ti["c"], send_sem=csend.at[k], recv_sem=crecv.at[k],
            device_id=(sibling,), device_id_type=MESH)

    def stage_copy(ti, slot, piece, stage):
        order = ORDERS[piece]
        lo, hi = ti["cuts"][piece]
        fixed = {order[i]: 0 for i in range(stage)}
        fixed[order[stage]] = 1
        src = ti["p"].at[(slot,) + block_index(fixed) + (slice(None), slice(lo, hi))]
        r = ti["r"][stage]
        dst = r.at[(slice(None),) * (len(r.shape) - 1) + (slice(lo, hi),)]
        return pltpu.make_async_remote_copy(
            src_ref=src, dst_ref=dst, send_sem=ssend.at[ti["k"], stage, piece], recv_sem=srecv.at[ti["k"], stage, piece],
            device_id=(partner[order[stage]],), device_id_type=MESH)

    def send_stage(ti, slot, stage):
        for piece in range(3):
            stage_copy(ti, slot, piece, stage).start()

    def take_stage(ti, slot, stage):
        for piece in range(3):
            stage_copy(ti, slot, piece, stage).wait()
        for piece in range(3):
            order = ORDERS[piece]
            lo, hi = ti["cuts"][piece]
            idx = (slot,) + block_index({order[i]: 0 for i in range(stage + 1)}) + (slice(None), slice(lo, hi))
            r = ti["r"][stage]
            ti["p"][idx] += r[(slice(None),) * (len(r.shape) - 1) + (slice(lo, hi),)]

    def out_copy(ti, it):
        slot = lax.rem(it, 2)
        lyr, n = layer_of(it), lax.rem(it, NIT)
        src = ti["p"].at[slot, 0, 0, 0]
        if ti["k"] == 0:
            dst = o2_hbm.at[lyr, pl.ds(pl.multiple_of(n * rows2, rows2), rows2)]
        else:
            dst = o1_hbm.at[lyr, :, pl.ds(pl.multiple_of(n * fw, fw), fw)]
        return pltpu.make_async_copy(src, dst, sem_out.at[ti["k"], slot])

    def first_half(ti, it, lhs, rhs):
        @pl.when(it > 0)
        def _():
            core_copy(ti).wait_send()
        ti["s"][...] = jnp.dot(lhs, rhs, preferred_element_type=F32)

        @pl.when(it > 0)
        def _():
            pl.semaphore_wait(credit.at[ti["k"]], 1)
        core_copy(ti).start()

    def second_half(ti, it, lhs, rhs):
        slot = lax.rem(it, 2)

        @pl.when(it > 1)
        def _():
            out_copy(ti, it - 2).wait()
        core_copy(ti).wait_recv()
        rows = ti["p"].shape[4]
        res = jnp.dot(lhs, rhs, preferred_element_type=F32)
        for b in range(8):
            sl = slice(b * rows, (b + 1) * rows)
            ti["p"][slot, b >> 2, (b >> 1) & 1, b & 1] = res[sl] + ti["c"][sl]

        @pl.when(it < total - 1)
        def _():
            pl.semaphore_signal(credit.at[ti["k"]], inc=1, device_id=(sibling,), device_id_type=MESH)
        send_stage(ti, slot, 0)

    def stage(ti, it, k):
        slot = lax.rem(it, 2)
        take_stage(ti, slot, k - 1)
        if k < 3:
            send_stage(ti, slot, k)
        else:
            out_copy(ti, it).start()

    def e_step(m, below):
        slot = lax.rem(m, 2)
        for c in e_copies(m):
            c.wait()
        vslot = lax.rem(lax.div(m, nsub), 2)
        col = lax.rem(m, nsub) * sub
        for c in range(2):
            rows = slice(c * half, (c + 1) * half)
            e = lax.dot_general(g[rows], wo[slot], (((1,), (1,)), ((), ())), preferred_element_type=F32)
            e = e.astype(BF).astype(F32)
            vv = (gelu_grad(u[slot, rows].astype(F32)) * e).astype(BF)
            v[vslot, rows, pl.ds(pl.multiple_of(col, sub), sub)] = vv
            if below:
                acc[rows] += lax.dot_general(vv, wi[slot], (((1,), (1,)), ((), ())), preferred_element_type=F32)

    barrier = pltpu.get_barrier_semaphore()
    for dev in (sibling,) + partner:
        pl.semaphore_signal(barrier, inc=1, device_id=(dev,), device_id_type=MESH)
    pl.semaphore_wait(barrier, 4)

    load_g = pltpu.make_async_copy(g_hbm, g, sem_g)
    load_g.start()
    start(at_copies(0))
    start(e_copies(0))
    start(ht_copies(layers - 1, 0))
    load_g.wait()
    acc[...] = g[...].astype(F32)
    ht_wait(0)

    t2, t1 = tiles[2], tiles[1]

    def body(it, carry):
        lyr, n = layer_of(it), lax.rem(it, NIT)
        lslot = lax.rem(lax.div(it, NIT), 2)
        slot = lax.rem(it, 2)
        live = it < total

        @pl.when(live)
        def _():
            at_wait(it)

            @pl.when(it + 1 < total)
            def _():
                start(at_copies(it + 1))
            first_half(t2, it, at[slot, 1], g[...])

        def run_e(m):
            @pl.when(m + 1 < total * nsub)
            def _():
                start(e_copies(m + 1))

            @pl.when(lyr > 0)
            def _():
                e_step(m, True)

            @pl.when(lyr == 0)
            def _():
                e_step(m, False)

        @pl.when(live)
        def _():
            run_e(it * nsub)

        @pl.when((it >= 2) & (it <= total + 1))
        def _():
            stage(t2, it - 2, 3)

        @pl.when((it >= 1) & (it <= total))
        def _():
            stage(t2, it - 1, 1)

        @pl.when((it >= 2) & (it <= total + 1))
        def _():
            stage(t1, it - 2, 2)

        @pl.when((it >= 1) & (it <= total))
        def _():
            prev = it - 1
            second_half(t1, prev, ht[lax.rem(lax.div(prev, NIT), 2), 0], v[lax.rem(prev, 2)])

        @pl.when(live)
        def _():
            for k in range(1, nsub):
                run_e(it * nsub + k)

            @pl.when((n == 1) & (lyr > 0))
            def _():
                start(ht_copies(lyr - 1, 1 - lslot))

            @pl.when((n == 0) & (it > 0))
            def _():
                ht_wait(lslot)
            first_half(t1, it, ht[lslot, 1], v[slot])

        @pl.when((it >= 2) & (it <= total + 1))
        def _():
            stage(t1, it - 2, 3)

        @pl.when((it >= 1) & (it <= total))
        def _():
            stage(t1, it - 1, 1)

        @pl.when((it >= 1) & (it <= total))
        def _():
            stage(t2, it - 1, 2)

        @pl.when(live)
        def _():
            second_half(t2, it, at[slot, 0], g[...])

            @pl.when((n == NIT - 1) & (lyr > 0))
            def _():
                new = acc[...].astype(BF)
                g[...] = new
                acc[...] = new.astype(F32)

        return carry

    lax.fori_loop(0, total + 2, body, 0)

    for ti in (t2, t1):
        core_copy(ti).wait_send()
        for it in (total - 2, total - 1):
            out_copy(ti, it).wait()


def backward(u, at, ht, g, w_in, w_out, cuts2, cuts1, sub=512):
    layers, t, ff = u.shape
    d = g.shape[1]
    rows2, rows1, fw = ff // 16 // NIT, d // 16, ff // NIT
    any_spec = pl.BlockSpec(memory_space=pl.ANY)
    scratch = [
        pltpu.VMEM((t, d), BF),
        pltpu.VMEM((t, d), F32),
        pltpu.VMEM((2, 2, 8 * rows1, t), BF),
        pltpu.VMEM((2, 2, 8 * rows2, t), BF),
        pltpu.VMEM((2, t, sub), BF),
        pltpu.VMEM((2, d, sub), BF),
        pltpu.VMEM((2, sub, d), BF),
        pltpu.VMEM((2, t, fw), BF),
        pltpu.VMEM((8 * rows2, d), F32),
        pltpu.VMEM((8 * rows1, fw), F32),
        pltpu.VMEM((8 * rows2, d), F32),
        pltpu.VMEM((8 * rows1, fw), F32),
        pltpu.VMEM((2, 2, 2, 2, rows2, d), F32),
        pltpu.VMEM((2, 2, 2, 2, rows1, fw), F32),
        pltpu.VMEM((2, 2, rows2, d), F32),
        pltpu.VMEM((2, rows2, d), F32),
        pltpu.VMEM((rows2, d), F32),
        pltpu.VMEM((2, 2, rows1, fw), F32),
        pltpu.VMEM((2, rows1, fw), F32),
        pltpu.VMEM((rows1, fw), F32),
        pltpu.SemaphoreType.DMA,
        pltpu.SemaphoreType.DMA((2,)),
        pltpu.SemaphoreType.DMA((2,)),
        pltpu.SemaphoreType.DMA((3, 2)),
        pltpu.SemaphoreType.DMA((2, 2)),
        pltpu.SemaphoreType.DMA((2,)),
        pltpu.SemaphoreType.DMA((2,)),
        pltpu.SemaphoreType.DMA((2, 3, 3)),
        pltpu.SemaphoreType.DMA((2, 3, 3)),
        pltpu.SemaphoreType.REGULAR((2,)),
    ]
    return pl.pallas_call(
        functools.partial(bwd_kernel, layers, cuts2, cuts1),
        in_specs=[any_spec] * 6,
        out_specs=[any_spec] * 2,
        out_shape=[
            jax.ShapeDtypeStruct((layers, d // 16, ff), F32),
            jax.ShapeDtypeStruct((layers, ff // 16, d), F32),
        ],
        scratch_shapes=scratch,
        compiler_params=pltpu.CompilerParams(
            collective_id=0, has_side_effects=True, vmem_limit_bytes=VMEM_LIMIT
        ),
        name="backward",
    )(u, at, ht, g, w_in, w_out)


def make(mesh, ftile=512, chunk=512, sub=512, cuts2=((0, 512), (512, 896), (896, 1280)), cuts1=((0, 256), (256, 640), (640, 1024))):
    data_size = mesh.shape["data"]

    def local_grads(tokens, targets, w_in, w_out):
        scale = (tokens.shape[0] * data_size) ** -0.5
        u, at, ht, g = forward(tokens, targets, w_in, w_out, scale, ftile, chunk)
        o1, o2 = backward(u, at, ht, g, w_in, w_out, cuts2, cuts1, sub)
        return o1, o2

    tok_spec = P("data", None)
    grad_spec = P(None, "data", None)
    return jax.shard_map(
        local_grads, mesh=mesh, in_specs=(tok_spec, tok_spec, P(), P()), out_specs=(grad_spec, grad_spec), check_vma=False
    )


SMALL_ARGS = dict(ftile=160, chunk=16, sub=128, cuts2=((0, 128), (128, 192), (192, 256)), cuts1=((0, 64), (64, 160), (160, 256)))


def solution(mesh):
    return make(mesh)
```
